32 devices in a mesh: rel: 2 (over y), row: 4 (over x, core), col: 4 (over z).
Axes of the slice: x: 2, y: 2, z: 4, core: 2. Of those that a mesh axis runs over, the one named last changes fastest.
Arguments:
- features: float32 [4, 16, 256, 128], P('rel', ('row', 'col')), may hold values from -6 to 6
- lap_tiles: bfloat16 [4, 4, 4, 16, 256, 256], P('rel', 'row', 'col'), may hold values from -0.046875 to 0.046875
- tile_rows: int32 [4, 4, 4, 16], P('rel', 'row', 'col'), may hold values from 0 to 3
- tile_cols: int32 [4, 4, 4, 16], P('rel', 'row', 'col'), may hold values from 0 to 3
- tile_count: int32 [4, 4, 4], P('rel', 'row', 'col'), may hold values from 2 to 16, as said below
- cheb_coefs: float32 [4, 5], P('rel'), may hold values from -1 to 1
- merging_weight: bfloat16 [512, 128], replicated, may hold values from -0.25 to 0.25
Outputs:
- merged_rows: float32 [16, 256, 128], P(('row', 'col'), 'rel')
The draws below stay inside these ranges and needn't reach their ends.
Inputs may be any that keep to these rules, and one draw needn't show every extreme that they name: Only the first tile_count slots of a device count; in every relation some device has 16 valid slots.
All inputs are finite; a program needn't handle non-finite values.
Results may differ from the reference program's by a relative error of at most 0.0063.
Values may be sent and summed in bfloat16 or wider, within the bound.
A program may use at most 64 MiB of HBM per device.

```python
import jax
import jax.numpy as jnp
from jax import lax

D = 128
TILE = 256
ORDERS = 4
PB = 1
TPD = 16
RELS = 4
PIECES = 16
PIECE_ROWS = 256
BLOCKS = 16
N_ROW = 4
N_COL = 4


def draw_tile_count(key, part):
    shift_key, pick_key = jax.random.split(key)
    levels = jnp.array([TPD, TPD // 2, TPD // 4, TPD // 8], dtype=jnp.int32)
    shifts = jax.random.randint(shift_key, (RELS, N_ROW * N_COL), 0, 4)
    counts = levels[shifts]
    chosen = jax.random.randint(pick_key, (RELS, 1), 0, N_ROW * N_COL)
    counts = jnp.where(jnp.arange(N_ROW * N_COL, dtype=jnp.int32)[None, :] == chosen, TPD, counts)
    return counts.reshape(RELS, N_ROW, N_COL).astype(jnp.int32)


def plant(drawn, own_key, low, high):
    shape = drawn.shape
    index_at = [jax.random.randint(jax.random.fold_in(own_key, axis), (), 0, shape[axis]) for axis in range(len(shape))]
    drawn = drawn.at[tuple(index_at)].set(low)
    longest = shape.index(max(shape))
    index_at[longest] = (index_at[longest] + 1) % shape[longest]
    return drawn.at[tuple(index_at)].set(high)


def block_levels(key, extent, shards, low, high):
    loudness = 1.0
    for dim, shards_of in shards:
        heights = jax.random.uniform(jax.random.fold_in(jax.random.fold_in(key, 6), dim), (shards_of,), jnp.float32, low / len(shards), high / len(shards))
        loudness = loudness * jnp.repeat(jnp.exp(heights), extent[dim] // shards_of).reshape((-1,) + (1,) * (len(extent) - 1 - dim))
    return loudness


def normal_values(stream_key, extent, deviation, bound, cuts=(), kind=jnp.bfloat16):
    level = block_levels(stream_key, extent, cuts, -0.22, 0.18) if cuts else 1.0
    drawn = jax.random.normal(stream_key, extent, jnp.float32) * deviation * level
    return jnp.minimum(jnp.maximum(drawn, -bound), bound).astype(kind)


def setup_inputs(seed: int = 0) -> dict:
    key_list = jax.random.split(jax.random.key(seed), 8)
    return {
        "features": normal_values(key_list[0], (RELS, PIECES, PIECE_ROWS, D), 1.0, 6.0, ((0, 2), (1, 16)), jnp.float32),
        "lap_tiles": normal_values(key_list[1], (RELS, N_ROW, N_COL, TPD, TILE, TILE), (4 * TILE * TPD // PB) ** -0.5, 0.046875, ((0, 2), (1, 4), (2, 4))),
        "tile_rows": plant(jax.random.randint(key_list[2], (RELS, N_ROW, N_COL, TPD), 0, N_COL * PB), jax.random.fold_in(key_list[2], 1), 0, (N_COL * PB) - 1).astype(jnp.int32),
        "tile_cols": plant(jax.random.randint(key_list[3], (RELS, N_ROW, N_COL, TPD), 0, N_ROW * PB), jax.random.fold_in(key_list[3], 1), 0, (N_ROW * PB) - 1).astype(jnp.int32),
        "tile_count": draw_tile_count(jax.random.fold_in(key_list[7], 71), 0),
        "cheb_coefs": jnp.clip(jax.random.uniform(key_list[5], (RELS, ORDERS + 1), jnp.float32, -1.0, 1.0) * block_levels(key_list[5], (RELS, ORDERS + 1), ((0, 2),), -0.4, 0.0), -1.0, 1.0),
        "merging_weight": normal_values(key_list[6], (RELS * D, D), (RELS * D) ** -0.5, 0.25),
    }


def shard_product(lap_tiles, tile_rows, tile_cols, tile_count, operand):
    blocks = operand.astype(jnp.float32).reshape(BLOCKS, TILE, D)
    col_index = jnp.arange(N_COL, dtype=jnp.int32)[:, None]
    slot_index = jnp.arange(TPD, dtype=jnp.int32)[None, :]

    def one_shard(inputs):
        shard_tiles, shard_rows, shard_cols, shard_count = inputs
        piece_index = (shard_cols // PB) * N_COL + col_index
        global_block = (piece_index * PB + shard_cols % PB).astype(jnp.int32)
        sources = blocks[global_block]
        products = jnp.einsum("cpab,cpbd->cpad", shard_tiles.astype(jnp.float32), sources,
                              precision=lax.Precision.HIGHEST)
        live_mask = (slot_index < shard_count[:, None]).astype(jnp.float32)
        products = products * live_mask[:, :, None, None]
        return jax.ops.segment_sum(products.reshape(N_COL * TPD, TILE, D),
                                   shard_rows.reshape(-1).astype(jnp.int32),
                                   num_segments=N_COL * PB)

    result = lax.map(one_shard, (lap_tiles, tile_rows, tile_cols, tile_count))
    return result.reshape(BLOCKS * TILE, D)


def reference(features, lap_tiles, tile_rows, tile_cols, tile_count, cheb_coefs, merging_weight):
    embeddings = []
    for relation in range(RELS):
        current = features[relation].reshape(BLOCKS * TILE, D)
        earlier = current
        embedding = cheb_coefs[relation, 0] * current
        for degree in range(1, ORDERS + 1):
            applied = shard_product(lap_tiles[relation], tile_rows[relation], tile_cols[relation],
                                    tile_count[relation], current.astype(jnp.bfloat16))
            if degree == 1:
                following = applied
            else:
                following = 2.0 * applied - earlier
            earlier, current = current, following
            embedding = embedding + cheb_coefs[relation, degree] * current
        embeddings.append(embedding.astype(jnp.bfloat16))
    joined = jnp.concatenate(embeddings, axis=1)
    merged_rows = jnp.dot(joined, merging_weight, preferred_element_type=jnp.float32)
    return merged_rows.reshape(PIECES, PIECE_ROWS, D)
```

```python
import functools

import jax
import jax.numpy as jnp
from jax import lax
from jax.experimental import pallas as pl
from jax.experimental.pallas import tpu as pltpu
from jax.sharding import PartitionSpec as P

ORDERS = 4
MESH = pl.DeviceIdType.MESH
VMEM_LIMIT = 60 * 1024 * 1024


def assemble_kernel(rows_ref, cols_ref, count_ref, tiles_ref, dense_ref, acc_ref):
    relation, block = pl.program_id(0), pl.program_id(1)
    slots, tile = tiles_ref.shape[1], tiles_ref.shape[2]
    acc_ref[...] = jnp.zeros_like(acc_ref)

    def add_slot(slot, carry):
        @pl.when((slot < count_ref[relation]) & (rows_ref[relation, slot] == block))
        def _():
            col = cols_ref[relation, slot]
            acc_ref[col] += tiles_ref[0, slot].astype(jnp.float32)

        return carry

    lax.fori_loop(0, slots, add_slot, 0)
    for col in range(acc_ref.shape[0]):
        dense_ref[0, 0, :, col * tile : (col + 1) * tile] = acc_ref[col].astype(dense_ref.dtype)


def assemble(lap_tiles, tile_rows, tile_cols, tile_count, row_count, col_count):
    rels, slots, tile, _ = lap_tiles.shape
    return pl.pallas_call(
        assemble_kernel,
        grid=(rels, col_count),
        out_shape=jax.ShapeDtypeStruct((rels, col_count, tile, row_count * tile), lap_tiles.dtype),
        in_specs=[
            pl.BlockSpec(memory_space=pltpu.SMEM),
            pl.BlockSpec(memory_space=pltpu.SMEM),
            pl.BlockSpec(memory_space=pltpu.SMEM),
            pl.BlockSpec((1, slots, tile, tile), lambda r, b: (r, 0, 0, 0)),
        ],
        out_specs=pl.BlockSpec((1, 1, tile, row_count * tile), lambda r, b: (r, b, 0, 0)),
        scratch_shapes=[pltpu.VMEM((row_count, tile, tile), jnp.float32)],
        compiler_params=pltpu.CompilerParams(vmem_limit_bytes=24 * 1024 * 1024),
    )(tile_rows, tile_cols, tile_count, lap_tiles)


def span(count, body, unroll_up_to=4):
    if count <= unroll_up_to:
        for index in range(count):
            body(index)
    else:
        lax.fori_loop(0, count, lambda index, carry: (body(index), carry)[1], 0)


def propagate_kernel(
    row_count, col_count, rel_count,
    features_ref, dense_ref, coefs_ref, weight_ref, merged_ref,
    lap_ref, gather_ref, partial_ref, arrived_ref, own_ref, current_ref, earlier_ref, total_ref,
    embed_ref, exchange_ref,
    load_sem, gather_send, gather_recv, scatter_send, scatter_recv, exchange_send, exchange_recv,
):
    rels, _, piece_rows, width = features_ref.shape
    my_row, my_col, my_rel = lax.axis_index("row"), lax.axis_index("col"), lax.axis_index("rel")
    part = piece_rows // rel_count

    def peer(me, offset, count):
        return lax.rem(me + offset, count)

    loads = [
        pltpu.make_async_copy(dense_ref.at[r], lap_ref.at[r], load_sem.at[r]) for r in range(rels)
    ]
    for load in loads:
        load.start()

    barrier = pltpu.get_barrier_semaphore()
    for axis, me, count in (("row", my_row, row_count), ("col", my_col, col_count), ("rel", my_rel, rel_count)):
        for offset in range(1, count):
            pl.semaphore_signal(
                barrier, inc=1, device_id={axis: peer(me, offset, count)}, device_id_type=MESH
            )
    pl.semaphore_wait(barrier, row_count + col_count + rel_count - 3)

    def gather_copy(order, r, source, target):
        return pltpu.make_async_remote_copy(
            src_ref=gather_ref.at[order, r, pl.ds(pl.multiple_of(source * piece_rows, piece_rows), piece_rows)],
            dst_ref=gather_ref.at[order, r, pl.ds(pl.multiple_of(source * piece_rows, piece_rows), piece_rows)],
            send_sem=gather_send.at[order, r, target],
            recv_sem=gather_recv.at[order, r, source],
            device_id={"row": target},
            device_id_type=MESH,
        )

    def scatter_copy(order, r, source, target):
        return pltpu.make_async_remote_copy(
            src_ref=partial_ref.at[order, r, target],
            dst_ref=arrived_ref.at[order, r, source],
            send_sem=scatter_send.at[order, r, target],
            recv_sem=scatter_recv.at[order, r, source],
            device_id={"col": target},
            device_id_type=MESH,
        )

    def exchange_copy(r, source, target):
        return pltpu.make_async_remote_copy(
            src_ref=embed_ref.at[r, target],
            dst_ref=exchange_ref.at[source, r],
            send_sem=exchange_send.at[r, target],
            recv_sem=exchange_recv.at[r, source],
            device_id={"rel": target},
            device_id_type=MESH,
        )

    def send_operand(order, r, value):
        gather_ref[order, r, pl.ds(pl.multiple_of(my_row * piece_rows, piece_rows), piece_rows)] = (
            value.astype(gather_ref.dtype)
        )
        for offset in range(1, row_count):
            gather_copy(order, r, my_row, peer(my_row, offset, row_count)).start()

    for r in range(rels):
        value = features_ref[r, 0]
        send_operand(0, r, value)
        current_ref[r] = value
        earlier_ref[r] = jnp.zeros_like(value)
        total_ref[r] = coefs_ref[r, 0] * value
    for load in loads:
        load.wait()

    def product(order, r, block):
        return jnp.dot(lap_ref[r, block], gather_ref[order, r], preferred_element_type=jnp.float32)

    def one_order(order, carry):
        for r in range(rels):
            for offset in range(1, row_count):
                gather_copy(order, r, peer(my_row, offset, row_count), my_row).wait_recv()

            def push(index):
                block = peer(my_col, index + 1, col_count)
                partial_ref[order, r, block] = product(order, r, block).astype(partial_ref.dtype)
                scatter_copy(order, r, my_col, block).start()

            span(col_count - 1, push)
            own_ref[r] = product(order, r, my_col)
        scale = jnp.where(order == 0, 1.0, 2.0).astype(jnp.float32)
        for r in range(rels):
            applied = own_ref[r]
            for offset in range(1, col_count):
                source = peer(my_col, offset, col_count)
                scatter_copy(order, r, source, my_col).wait_recv()
                applied = applied + arrived_ref[order, r, source].astype(jnp.float32)
            following = scale * applied - earlier_ref[r]

            @pl.when(order + 1 < ORDERS)
            def _():
                send_operand(order + 1, r, following)

            earlier_ref[r] = current_ref[r]
            current_ref[r] = following
            total_ref[r] += coefs_ref[r, order + 1] * following
        return carry

    lax.fori_loop(0, ORDERS, one_order, 0)

    for r in range(rels):
        embedded = total_ref[r].astype(embed_ref.dtype)
        embed_ref[r] = embedded.reshape(rel_count, part, width)
        exchange_ref[my_rel, r] = embed_ref[r, my_rel]
        for offset in range(1, rel_count):
            exchange_copy(r, my_rel, peer(my_rel, offset, rel_count)).start()

    def drain(order, carry):
        for r in range(rels):
            for offset in range(1, row_count):
                gather_copy(order, r, my_row, peer(my_row, offset, row_count)).wait_send()
            for offset in range(1, col_count):
                scatter_copy(order, r, my_col, peer(my_col, offset, col_count)).wait_send()
        return carry

    lax.fori_loop(0, ORDERS, drain, 0)
    for r in range(rels):
        for offset in range(1, rel_count):
            other = peer(my_rel, offset, rel_count)
            exchange_copy(r, my_rel, other).wait_send()
            exchange_copy(r, other, my_rel).wait_recv()
    merged = jnp.zeros((part, width), jnp.float32)
    for group in range(rel_count):
        for r in range(rels):
            start = (group * rels + r) * width
            merged = merged + jnp.dot(
                exchange_ref[group, r], weight_ref[start : start + width, :],
                preferred_element_type=jnp.float32,
            )
    merged_ref[0] = merged


def local(features, lap_tiles, tile_rows, tile_cols, tile_count, cheb_coefs, merging_weight):
    row_count, col_count, rel_count = (lax.axis_size(name) for name in ("row", "col", "rel"))
    rels, _, piece_rows, width = features.shape
    part = piece_rows // rel_count
    dense = assemble(
        lap_tiles[:, 0, 0], tile_rows[:, 0, 0], tile_cols[:, 0, 0], tile_count[:, 0, 0], row_count, col_count
    )
    vmem = pl.BlockSpec(memory_space=pltpu.VMEM)
    half = jnp.bfloat16
    dma = pltpu.SemaphoreType.DMA
    return pl.pallas_call(
        functools.partial(propagate_kernel, row_count, col_count, rel_count),
        out_shape=jax.ShapeDtypeStruct((1, part, width), jnp.float32),
        in_specs=[vmem, pl.BlockSpec(memory_space=pl.ANY), pl.BlockSpec(memory_space=pltpu.SMEM), vmem],
        out_specs=vmem,
        scratch_shapes=[
            pltpu.VMEM(dense.shape, dense.dtype),
            pltpu.VMEM((ORDERS, rels, row_count * piece_rows, width), half),
            pltpu.VMEM((ORDERS, rels, col_count, piece_rows, width), half),
            pltpu.VMEM((ORDERS, rels, col_count, piece_rows, width), half),
            pltpu.VMEM((rels, piece_rows, width), jnp.float32),
            pltpu.VMEM((rels, piece_rows, width), jnp.float32),
            pltpu.VMEM((rels, piece_rows, width), jnp.float32),
            pltpu.VMEM((rels, piece_rows, width), jnp.float32),
            pltpu.VMEM((rels, rel_count, part, width), half),
            pltpu.VMEM((rel_count, rels, part, width), half),
            dma((rels,)),
            dma((ORDERS, rels, row_count)),
            dma((ORDERS, rels, row_count)),
            dma((ORDERS, rels, col_count)),
            dma((ORDERS, rels, col_count)),
            dma((rels, rel_count)),
            dma((rels, rel_count)),
        ],
        compiler_params=pltpu.CompilerParams(
            collective_id=0, has_side_effects=True, vmem_limit_bytes=VMEM_LIMIT
        ),
    )(features, dense, cheb_coefs, merging_weight)


def solution(mesh):
    placed = (
        P("rel", ("row", "col"), None, None),
        P("rel", "row", "col", None, None, None),
        P("rel", "row", "col", None),
        P("rel", "row", "col", None),
        P("rel", "row", "col"),
        P("rel", None),
        P(),
    )
    return jax.shard_map(
        local, mesh=mesh, in_specs=placed, out_specs=P(("row", "col"), "rel", None), check_vma=False
    )
```

```python
import functools

import jax
import jax.numpy as jnp
from jax import lax
from jax.experimental import pallas as pl
from jax.experimental.pallas import tpu as pltpu
from jax.sharding import PartitionSpec as P

ORDERS = 4
MESH = pl.DeviceIdType.MESH
VMEM_LIMIT = 60 * 1024 * 1024


def assemble_kernel(rows_ref, cols_ref, count_ref, tiles_ref, dense_ref, acc_ref):
    relation, block = pl.program_id(0), pl.program_id(1)
    slots, tile = tiles_ref.shape[1], tiles_ref.shape[2]
    acc_ref[...] = jnp.zeros_like(acc_ref)

    def add_slot(slot, carry):
        @pl.when((slot < count_ref[relation]) & (rows_ref[relation, slot] == block))
        def _():
            col = cols_ref[relation, slot]
            acc_ref[col] += tiles_ref[0, slot].astype(jnp.float32)

        return carry

    lax.fori_loop(0, slots, add_slot, 0)
    for col in range(acc_ref.shape[0]):
        dense_ref[0, 0, :, col * tile : (col + 1) * tile] = acc_ref[col].astype(dense_ref.dtype)


def assemble(lap_tiles, tile_rows, tile_cols, tile_count, row_count, col_count):
    rels, slots, tile, _ = lap_tiles.shape
    return pl.pallas_call(
        assemble_kernel,
        grid=(rels, col_count),
        out_shape=jax.ShapeDtypeStruct((rels, col_count, tile, row_count * tile), lap_tiles.dtype),
        in_specs=[
            pl.BlockSpec(memory_space=pltpu.SMEM),
            pl.BlockSpec(memory_space=pltpu.SMEM),
            pl.BlockSpec(memory_space=pltpu.SMEM),
            pl.BlockSpec((1, slots, tile, tile), lambda r, b: (r, 0, 0, 0)),
        ],
        out_specs=pl.BlockSpec((1, 1, tile, row_count * tile), lambda r, b: (r, b, 0, 0)),
        scratch_shapes=[pltpu.VMEM((row_count, tile, tile), jnp.float32)],
        compiler_params=pltpu.CompilerParams(vmem_limit_bytes=24 * 1024 * 1024),
    )(tile_rows, tile_cols, tile_count, lap_tiles)


def span(count, body, unroll_up_to=4):
    if count <= unroll_up_to:
        for index in range(count):
            body(index)
    else:
        lax.fori_loop(0, count, lambda index, carry: (body(index), carry)[1], 0)


def propagate_kernel(
    row_count, col_count, rel_count,
    features_hbm, dense_ref, coefs_ref, weight_hbm, merged_ref,
    features_ref, weight_ref, lap_ref, gather_ref, partial_ref, arrived_ref, own_ref, current_ref, earlier_ref, total_ref,
    embed_ref, exchange_ref,
    load_sem, features_sem, weight_sem, gather_send, gather_recv, scatter_send, scatter_recv, exchange_send, exchange_recv,
):
    rels, _, piece_rows, width = features_ref.shape
    my_row, my_col, my_rel = lax.axis_index("row"), lax.axis_index("col"), lax.axis_index("rel")
    part = piece_rows // rel_count

    def peer(me, offset, count):
        return lax.rem(me + offset, count)

    features_load = pltpu.make_async_copy(features_hbm, features_ref, features_sem)
    features_load.start()
    loads = [
        pltpu.make_async_copy(dense_ref.at[r], lap_ref.at[r], load_sem.at[r]) for r in range(rels)
    ]
    for load in loads:
        load.start()
    weight_load = pltpu.make_async_copy(weight_hbm, weight_ref, weight_sem)
    weight_load.start()

    barrier = pltpu.get_barrier_semaphore()
    for axis, me, count in (("row", my_row, row_count), ("col", my_col, col_count), ("rel", my_rel, rel_count)):
        for offset in range(1, count):
            pl.semaphore_signal(
                barrier, inc=1, device_id={axis: peer(me, offset, count)}, device_id_type=MESH
            )
    pl.semaphore_wait(barrier, row_count + col_count + rel_count - 3)

    def gather_copy(order, r, source, target):
        return pltpu.make_async_remote_copy(
            src_ref=gather_ref.at[order, r, pl.ds(pl.multiple_of(source * piece_rows, piece_rows), piece_rows)],
            dst_ref=gather_ref.at[order, r, pl.ds(pl.multiple_of(source * piece_rows, piece_rows), piece_rows)],
            send_sem=gather_send.at[order, r, target],
            recv_sem=gather_recv.at[order, r, source],
            device_id={"row": target},
            device_id_type=MESH,
        )

    def scatter_copy(order, r, source, target):
        return pltpu.make_async_remote_copy(
            src_ref=partial_ref.at[order, r, target],
            dst_ref=arrived_ref.at[order, r, source],
            send_sem=scatter_send.at[order, r, target],
            recv_sem=scatter_recv.at[order, r, source],
            device_id={"col": target},
            device_id_type=MESH,
        )

    def exchange_copy(r, source, target):
        return pltpu.make_async_remote_copy(
            src_ref=embed_ref.at[r, target],
            dst_ref=exchange_ref.at[source, r],
            send_sem=exchange_send.at[r, target],
            recv_sem=exchange_recv.at[r, source],
            device_id={"rel": target},
            device_id_type=MESH,
        )

    def send_operand(order, r, value):
        gather_ref[order, r, pl.ds(pl.multiple_of(my_row * piece_rows, piece_rows), piece_rows)] = (
            value.astype(gather_ref.dtype)
        )
        for offset in range(1, row_count):
            gather_copy(order, r, my_row, peer(my_row, offset, row_count)).start()

    features_load.wait()
    for r in range(rels):
        send_operand(0, r, features_ref[r, 0])
    for r in range(rels):
        value = features_ref[r, 0]
        current_ref[r] = value
        earlier_ref[r] = jnp.zeros_like(value)
        total_ref[r] = coefs_ref[r, 0] * value

    def product(order, r, block):
        return jnp.dot(lap_ref[r, block], gather_ref[order, r], preferred_element_type=jnp.float32)

    def push_partials(order, r):
        for offset in range(1, row_count):
            gather_copy(order, r, peer(my_row, offset, row_count), my_row).wait_recv()

        def push(index):
            offset = 1 + (col_count // 2 - 1 + index) % (col_count - 1)
            block = peer(my_col, offset, col_count)
            partial_ref[order, r, block] = product(order, r, block).astype(partial_ref.dtype)
            scatter_copy(order, r, my_col, block).start()

        span(col_count - 1, push)
        own_ref[r] = product(order, r, my_col)

    def advance(order, r, send):
        applied = own_ref[r]
        for offset in range(1, col_count):
            source = peer(my_col, offset, col_count)
            scatter_copy(order, r, source, my_col).wait_recv()
            applied = applied + arrived_ref[order, r, source].astype(jnp.float32)
        scale = jnp.where(order == 0, 1.0, 2.0).astype(jnp.float32)
        following = scale * applied - earlier_ref[r]
        if send:
            send_operand(order + 1, r, following)
        earlier_ref[r] = current_ref[r]
        current_ref[r] = following
        total_ref[r] += coefs_ref[r, order + 1] * following

    for r in range(rels):
        loads[r].wait()
        push_partials(0, r)

    def one_order(order, carry):
        for r in range(rels):
            advance(order, r, True)
            push_partials(order + 1, r)
        return carry

    lax.fori_loop(0, ORDERS - 1, one_order, 0)

    for r in range(rels):
        advance(ORDERS - 1, r, False)
        embedded = total_ref[r].astype(embed_ref.dtype)
        embed_ref[r] = embedded.reshape(rel_count, part, width)
        exchange_ref[my_rel, r] = embed_ref[r, my_rel]
        for offset in range(1, rel_count):
            exchange_copy(r, my_rel, peer(my_rel, offset, rel_count)).start()

    def drain(order, carry):
        for r in range(rels):
            for offset in range(1, row_count):
                gather_copy(order, r, my_row, peer(my_row, offset, row_count)).wait_send()
            for offset in range(1, col_count):
                scatter_copy(order, r, my_col, peer(my_col, offset, col_count)).wait_send()
        return carry

    lax.fori_loop(0, ORDERS, drain, 0)
    for r in range(rels):
        for offset in range(1, rel_count):
            other = peer(my_rel, offset, rel_count)
            exchange_copy(r, my_rel, other).wait_send()
            exchange_copy(r, other, my_rel).wait_recv()
    weight_load.wait()
    merged = jnp.zeros((part, width), jnp.float32)
    for group in range(rel_count):
        for r in range(rels):
            start = (group * rels + r) * width
            merged = merged + jnp.dot(
                exchange_ref[group, r], weight_ref[start : start + width, :],
                preferred_element_type=jnp.float32,
            )
    merged_ref[0] = merged


def local(features, lap_tiles, tile_rows, tile_cols, tile_count, cheb_coefs, merging_weight):
    row_count, col_count, rel_count = (lax.axis_size(name) for name in ("row", "col", "rel"))
    rels, _, piece_rows, width = features.shape
    part = piece_rows // rel_count
    dense = assemble(
        lap_tiles[:, 0, 0], tile_rows[:, 0, 0], tile_cols[:, 0, 0], tile_count[:, 0, 0], row_count, col_count
    )
    vmem = pl.BlockSpec(memory_space=pltpu.VMEM)
    anywhere = pl.BlockSpec(memory_space=pl.ANY)
    half = jnp.bfloat16
    dma = pltpu.SemaphoreType.DMA
    return pl.pallas_call(
        functools.partial(propagate_kernel, row_count, col_count, rel_count),
        out_shape=jax.ShapeDtypeStruct((1, part, width), jnp.float32),
        in_specs=[anywhere, anywhere, pl.BlockSpec(memory_space=pltpu.SMEM), anywhere],
        out_specs=vmem,
        scratch_shapes=[
            pltpu.VMEM(features.shape, features.dtype),
            pltpu.VMEM(merging_weight.shape, merging_weight.dtype),
            pltpu.VMEM(dense.shape, dense.dtype),
            pltpu.VMEM((ORDERS, rels, row_count * piece_rows, width), half),
            pltpu.VMEM((ORDERS, rels, col_count, piece_rows, width), half),
            pltpu.VMEM((ORDERS, rels, col_count, piece_rows, width), half),
            pltpu.VMEM((rels, piece_rows, width), jnp.float32),
            pltpu.VMEM((rels, piece_rows, width), jnp.float32),
            pltpu.VMEM((rels, piece_rows, width), jnp.float32),
            pltpu.VMEM((rels, piece_rows, width), jnp.float32),
            pltpu.VMEM((rels, rel_count, part, width), half),
            pltpu.VMEM((rel_count, rels, part, width), half),
            dma((rels,)),
            dma,
            dma,
            dma((ORDERS, rels, row_count)),
            dma((ORDERS, rels, row_count)),
            dma((ORDERS, rels, col_count)),
            dma((ORDERS, rels, col_count)),
            dma((rels, rel_count)),
            dma((rels, rel_count)),
        ],
        compiler_params=pltpu.CompilerParams(
            collective_id=0, has_side_effects=True, vmem_limit_bytes=VMEM_LIMIT
        ),
    )(features, dense, cheb_coefs, merging_weight)


def solution(mesh):
    placed = (
        P("rel", ("row", "col"), None, None),
        P("rel", "row", "col", None, None, None),
        P("rel", "row", "col", None),
        P("rel", "row", "col", None),
        P("rel", "row", "col"),
        P("rel", None),
        P(),
    )
    return jax.shard_map(
        local, mesh=mesh, in_specs=placed, out_specs=P(("row", "col"), "rel", None), check_vma=False
    )
```

```python
import functools

import jax
import jax.numpy as jnp
from jax import lax
from jax.experimental import pallas as pl
from jax.experimental.pallas import tpu as pltpu
from jax.sharding import PartitionSpec as P

ORDERS = 4
MESH = pl.DeviceIdType.MESH
VMEM_LIMIT = 60 * 1024 * 1024


def assemble_kernel(
    rows_hbm, cols_hbm, count_hbm, tiles_ref, dense_ref, acc_ref, rows_ref, cols_ref, count_ref, index_sem
):
    relation, block = pl.program_id(0), pl.program_id(1)

    @pl.when((relation == 0) & (block == 0))
    def _():
        loads = [
            pltpu.make_async_copy(source, target, index_sem.at[index])
            for index, (source, target) in enumerate(
                ((rows_hbm, rows_ref), (cols_hbm, cols_ref), (count_hbm, count_ref))
            )
        ]
        for load in loads:
            load.start()
        for load in loads:
            load.wait()

    slots, tile = tiles_ref.shape[1], tiles_ref.shape[2]
    acc_ref[...] = jnp.zeros_like(acc_ref)

    def add_slot(slot, carry):
        @pl.when((slot < count_ref[relation]) & (rows_ref[relation, slot] == block))
        def _():
            col = cols_ref[relation, slot]
            acc_ref[col] += tiles_ref[0, slot].astype(jnp.float32)

        return carry

    lax.fori_loop(0, slots, add_slot, 0)
    for col in range(acc_ref.shape[0]):
        dense_ref[0, 0, :, col * tile : (col + 1) * tile] = acc_ref[col].astype(dense_ref.dtype)


def assemble(lap_tiles, tile_rows, tile_cols, tile_count, row_count, col_count):
    rels, slots, tile, _ = lap_tiles.shape
    return pl.pallas_call(
        assemble_kernel,
        grid=(rels, col_count),
        out_shape=jax.ShapeDtypeStruct((rels, col_count, tile, row_count * tile), lap_tiles.dtype),
        in_specs=[
            pl.BlockSpec(memory_space=pl.ANY),
            pl.BlockSpec(memory_space=pl.ANY),
            pl.BlockSpec(memory_space=pl.ANY),
            pl.BlockSpec((1, slots, tile, tile), lambda r, b: (r, 0, 0, 0)),
        ],
        out_specs=pl.BlockSpec((1, 1, tile, row_count * tile), lambda r, b: (r, b, 0, 0)),
        scratch_shapes=[
            pltpu.VMEM((row_count, tile, tile), jnp.float32),
            pltpu.SMEM(tile_rows.shape, tile_rows.dtype),
            pltpu.SMEM(tile_cols.shape, tile_cols.dtype),
            pltpu.SMEM(tile_count.shape, tile_count.dtype),
            pltpu.SemaphoreType.DMA((3,)),
        ],
        compiler_params=pltpu.CompilerParams(vmem_limit_bytes=24 * 1024 * 1024),
    )(tile_rows, tile_cols, tile_count, lap_tiles)


def span(count, body, unroll_up_to=4):
    if count <= unroll_up_to:
        for index in range(count):
            body(index)
    else:
        lax.fori_loop(0, count, lambda index, carry: (body(index), carry)[1], 0)


def propagate_kernel(
    row_count, col_count, rel_count,
    features_hbm, dense_ref, coefs_hbm, weight_hbm, merged_ref,
    coefs_ref, features_ref, weight_ref, lap_ref, gather_ref, partial_ref, arrived_ref, own_ref, current_ref, earlier_ref, total_ref,
    embed_ref, exchange_ref,
    load_sem, coefs_sem, features_sem, weight_sem, gather_send, gather_recv, scatter_send, scatter_recv, exchange_send, exchange_recv,
):
    rels, _, piece_rows, width = features_ref.shape
    my_row, my_col, my_rel = lax.axis_index("row"), lax.axis_index("col"), lax.axis_index("rel")
    part = piece_rows // rel_count

    def peer(me, offset, count):
        return lax.rem(me + offset, count)

    features_load = pltpu.make_async_copy(features_hbm, features_ref, features_sem)
    features_load.start()
    coefs_load = pltpu.make_async_copy(coefs_hbm, coefs_ref, coefs_sem)
    coefs_load.start()
    loads = [
        pltpu.make_async_copy(dense_ref.at[r], lap_ref.at[r], load_sem.at[r]) for r in range(rels)
    ]
    for load in loads:
        load.start()
    weight_load = pltpu.make_async_copy(weight_hbm, weight_ref, weight_sem)
    weight_load.start()

    barrier = pltpu.get_barrier_semaphore()
    for axis, me, count in (("row", my_row, row_count), ("col", my_col, col_count), ("rel", my_rel, rel_count)):
        for offset in range(1, count):
            pl.semaphore_signal(
                barrier, inc=1, device_id={axis: peer(me, offset, count)}, device_id_type=MESH
            )
    pl.semaphore_wait(barrier, row_count + col_count + rel_count - 3)

    def gather_copy(order, r, source, target):
        return pltpu.make_async_remote_copy(
            src_ref=gather_ref.at[order, r, pl.ds(pl.multiple_of(source * piece_rows, piece_rows), piece_rows)],
            dst_ref=gather_ref.at[order, r, pl.ds(pl.multiple_of(source * piece_rows, piece_rows), piece_rows)],
            send_sem=gather_send.at[order, r, target],
            recv_sem=gather_recv.at[order, r, source],
            device_id={"row": target},
            device_id_type=MESH,
        )

    def scatter_copy(order, r, source, target):
        return pltpu.make_async_remote_copy(
            src_ref=partial_ref.at[order, r, target],
            dst_ref=arrived_ref.at[order, r, source],
            send_sem=scatter_send.at[order, r, target],
            recv_sem=scatter_recv.at[order, r, source],
            device_id={"col": target},
            device_id_type=MESH,
        )

    def exchange_copy(r, source, target):
        return pltpu.make_async_remote_copy(
            src_ref=embed_ref.at[r, target],
            dst_ref=exchange_ref.at[source, r],
            send_sem=exchange_send.at[r, target],
            recv_sem=exchange_recv.at[r, source],
            device_id={"rel": target},
            device_id_type=MESH,
        )

    def send_operand(order, r, value):
        gather_ref[order, r, pl.ds(pl.multiple_of(my_row * piece_rows, piece_rows), piece_rows)] = (
            value.astype(gather_ref.dtype)
        )
        for offset in range(1, row_count):
            gather_copy(order, r, my_row, peer(my_row, offset, row_count)).start()

    features_load.wait()
    for r in range(rels):
        send_operand(0, r, features_ref[r, 0])
    coefs_load.wait()
    for r in range(rels):
        value = features_ref[r, 0]
        current_ref[r] = value
        earlier_ref[r] = jnp.zeros_like(value)
        total_ref[r] = coefs_ref[r, 0] * value

    def product(order, r, block):
        return jnp.dot(lap_ref[r, block], gather_ref[order, r], preferred_element_type=jnp.float32)

    def push_partials(order, r):
        for offset in range(1, row_count):
            gather_copy(order, r, peer(my_row, offset, row_count), my_row).wait_recv()

        def push(index):
            offset = 1 + (col_count // 2 - 1 + index) % (col_count - 1)
            block = peer(my_col, offset, col_count)
            partial_ref[order, r, block] = product(order, r, block).astype(partial_ref.dtype)
            scatter_copy(order, r, my_col, block).start()

        span(col_count - 1, push)
        own_ref[r] = product(order, r, my_col)

    def advance(order, r, send):
        applied = own_ref[r]
        for offset in range(1, col_count):
            source = peer(my_col, offset, col_count)
            scatter_copy(order, r, source, my_col).wait_recv()
            applied = applied + arrived_ref[order, r, source].astype(jnp.float32)
        scale = jnp.where(order == 0, 1.0, 2.0).astype(jnp.float32)
        following = scale * applied - earlier_ref[r]
        if send:
            send_operand(order + 1, r, following)
        earlier_ref[r] = current_ref[r]
        current_ref[r] = following
        total_ref[r] += coefs_ref[r, order + 1] * following

    for r in range(rels):
        loads[r].wait()
        push_partials(0, r)

    def one_order(order, carry):
        for r in range(rels):
            advance(order, r, True)
            push_partials(order + 1, r)
        return carry

    lax.fori_loop(0, ORDERS - 1, one_order, 0)

    for r in range(rels):
        advance(ORDERS - 1, r, False)
        embedded = total_ref[r].astype(embed_ref.dtype)
        embed_ref[r] = embedded.reshape(rel_count, part, width)
        exchange_ref[my_rel, r] = embed_ref[r, my_rel]
        for offset in range(1, rel_count):
            exchange_copy(r, my_rel, peer(my_rel, offset, rel_count)).start()

    def drain(order, carry):
        for r in range(rels):
            for offset in range(1, row_count):
                gather_copy(order, r, my_row, peer(my_row, offset, row_count)).wait_send()
            for offset in range(1, col_count):
                scatter_copy(order, r, my_col, peer(my_col, offset, col_count)).wait_send()
        return carry

    lax.fori_loop(0, ORDERS, drain, 0)
    for r in range(rels):
        for offset in range(1, rel_count):
            other = peer(my_rel, offset, rel_count)
            exchange_copy(r, my_rel, other).wait_send()
            exchange_copy(r, other, my_rel).wait_recv()
    weight_load.wait()
    merged = jnp.zeros((part, width), jnp.float32)
    for group in range(rel_count):
        for r in range(rels):
            start = (group * rels + r) * width
            merged = merged + jnp.dot(
                exchange_ref[group, r], weight_ref[start : start + width, :],
                preferred_element_type=jnp.float32,
            )
    merged_ref[0] = merged


def local(features, lap_tiles, tile_rows, tile_cols, tile_count, cheb_coefs, merging_weight):
    row_count, col_count, rel_count = (lax.axis_size(name) for name in ("row", "col", "rel"))
    rels, _, piece_rows, width = features.shape
    part = piece_rows // rel_count
    dense = assemble(
        lap_tiles[:, 0, 0], tile_rows[:, 0, 0], tile_cols[:, 0, 0], tile_count[:, 0, 0], row_count, col_count
    )
    vmem = pl.BlockSpec(memory_space=pltpu.VMEM)
    anywhere = pl.BlockSpec(memory_space=pl.ANY)
    half = jnp.bfloat16
    dma = pltpu.SemaphoreType.DMA
    return pl.pallas_call(
        functools.partial(propagate_kernel, row_count, col_count, rel_count),
        out_shape=jax.ShapeDtypeStruct((1, part, width), jnp.float32),
        in_specs=[anywhere] * 4,
        out_specs=vmem,
        scratch_shapes=[
            pltpu.SMEM(cheb_coefs.shape, cheb_coefs.dtype),
            pltpu.VMEM(features.shape, features.dtype),
            pltpu.VMEM(merging_weight.shape, merging_weight.dtype),
            pltpu.VMEM(dense.shape, dense.dtype),
            pltpu.VMEM((ORDERS, rels, row_count * piece_rows, width), half),
            pltpu.VMEM((ORDERS, rels, col_count, piece_rows, width), half),
            pltpu.VMEM((ORDERS, rels, col_count, piece_rows, width), half),
            pltpu.VMEM((rels, piece_rows, width), jnp.float32),
            pltpu.VMEM((rels, piece_rows, width), jnp.float32),
            pltpu.VMEM((rels, piece_rows, width), jnp.float32),
            pltpu.VMEM((rels, piece_rows, width), jnp.float32),
            pltpu.VMEM((rels, rel_count, part, width), half),
            pltpu.VMEM((rel_count, rels, part, width), half),
            dma((rels,)),
            dma,
            dma,
            dma,
            dma((ORDERS, rels, row_count)),
            dma((ORDERS, rels, row_count)),
            dma((ORDERS, rels, col_count)),
            dma((ORDERS, rels, col_count)),
            dma((rels, rel_count)),
            dma((rels, rel_count)),
        ],
        compiler_params=pltpu.CompilerParams(
            collective_id=0, has_side_effects=True, vmem_limit_bytes=VMEM_LIMIT
        ),
    )(features, dense, cheb_coefs, merging_weight)


def solution(mesh):
    placed = (
        P("rel", ("row", "col"), None, None),
        P("rel", "row", "col", None, None, None),
        P("rel", "row", "col", None),
        P("rel", "row", "col", None),
        P("rel", "row", "col"),
        P("rel", None),
        P(),
    )
    return jax.shard_map(
        local, mesh=mesh, in_specs=placed, out_specs=P(("row", "col"), "rel", None), check_vma=False
    )
```
